32 devices in a mesh: dp: 4 (over y, z), tp: 8 (over x, core).
Axes of the slice: x: 4, y: 2, z: 2, core: 2. Of those that a mesh axis runs over, the one named last changes fastest.
The devices are a block of a 4x4x8 slice.
Arguments:
- hidden: bfloat16 [24, 512, 4096], P('dp', 'tp'), parts along dimension 0
- positions: int32 [24, 512], P('dp', 'tp'), parts along dimension 0
- doc_ids: int32 [24, 512], P('dp', 'tp'), parts along dimension 0
- norm_gain: bfloat16 [4096], replicated
- w_query: bfloat16 [4096, 4096], P(None, 'tp')
- w_key: bfloat16 [4096, 1024], P(None, 'tp')
- w_value: bfloat16 [4096, 1024], P(None, 'tp')
- w_out: bfloat16 [4096, 4096], P('tp')
- grad_out: bfloat16 [24, 512, 4096], P('dp', 'tp'), parts along dimension 0
Outputs:
- output 1: bfloat16 [24, 512, 4096], P('dp', 'tp'), parts along dimension 0
- output 2: bfloat16 [24, 512, 4096], P('dp', 'tp'), parts along dimension 0
- output 3: float32 [16384], P('dp'), parts along dimension 0
- output 4: float32 [16384, 4096], P('dp', 'tp'), parts along dimension 0
- output 5: float32 [16384, 1024], P('dp', 'tp'), parts along dimension 0
- output 6: float32 [16384, 1024], P('dp', 'tp'), parts along dimension 0
- output 7: float32 [16384, 4096], P(('dp', 'tp')), parts along dimension 0
There are 4 independent parts. The reference program is written for one: setup_inputs(seed, part) draws one part's arguments, and reference() takes and returns one part's arrays. A program takes and returns all parts, laid end to end along the dimension named above; an argument that names none is the same for every part.
All inputs are finite; a program needn't handle non-finite values.
Results may differ from the reference program's by a relative error of at most 0.0098466.
Values are sent between devices in bfloat16 or wider.
A program may use at most 768 MiB of HBM per device.

```python
import jax
import jax.numpy as jnp
from jax import lax

BATCH_ROWS = 6
SEQ_LEN = 512
MODEL_DIM = 4096
NUM_HEADS = 32
NUM_KV_HEADS = 8
HEAD_DIM = 128
NORM_EPS = 1e-5
ROPE_BASE = 10000.0


def draw_documents(doc_key):
    doc_mean = max(4, SEQ_LEN // 8)
    token_idx = jnp.arange(SEQ_LEN, dtype=jnp.int32)
    starts = jax.random.randint(doc_key, (BATCH_ROWS, SEQ_LEN), 0, doc_mean) == 0
    starts = starts | (token_idx == 0)[None, :]
    doc_ids = jnp.cumsum(starts.astype(jnp.int32), axis=1) - 1
    begins = lax.cummax(jnp.where(starts, token_idx[None, :], 0), axis=1)
    return (token_idx[None, :] - begins).astype(jnp.int32), doc_ids.astype(jnp.int32)


def setup_inputs(seed: int = 0, part: int = 0) -> dict:
    part_key = jax.random.fold_in(jax.random.key(seed), part)
    shared_key = jax.random.key(seed + 1)
    k_hidden, k_grad, k_doc = jax.random.split(part_key, 3)
    k_gain, k_query, k_key, k_value, k_out = jax.random.split(shared_key, 5)
    positions, doc_ids = draw_documents(k_doc)
    in_scale = MODEL_DIM ** -0.5
    out_scale = 2.0 * (NUM_HEADS * HEAD_DIM) ** -0.5
    q_width = NUM_HEADS * HEAD_DIM
    kv_width = NUM_KV_HEADS * HEAD_DIM
    return {
        'hidden': jax.random.normal(k_hidden, (BATCH_ROWS, SEQ_LEN, MODEL_DIM), jnp.float32).astype(jnp.bfloat16),
        'positions': positions,
        'doc_ids': doc_ids,
        'norm_gain': (1.0 + 0.3 * jax.random.normal(k_gain, (MODEL_DIM,), jnp.float32)).astype(jnp.bfloat16),
        'w_query': (in_scale * jax.random.normal(k_query, (MODEL_DIM, q_width), jnp.float32)).astype(jnp.bfloat16),
        'w_key': (in_scale * jax.random.normal(k_key, (MODEL_DIM, kv_width), jnp.float32)).astype(jnp.bfloat16),
        'w_value': (in_scale * jax.random.normal(k_value, (MODEL_DIM, kv_width), jnp.float32)).astype(jnp.bfloat16),
        'w_out': (out_scale * jax.random.normal(k_out, (q_width, MODEL_DIM), jnp.float32)).astype(jnp.bfloat16),
        'grad_out': jax.random.normal(k_grad, (BATCH_ROWS, SEQ_LEN, MODEL_DIM), jnp.float32).astype(jnp.bfloat16),
    }


def snap_bf16(values):
    return values + lax.stop_gradient(values.astype(jnp.bfloat16).astype(values.dtype) - values)


def rotate_pairs(values, cos_tab, sin_tab):
    pair_view = values.reshape(values.shape[:-1] + (HEAD_DIM // 2, 2))
    even_part = pair_view[..., 0]
    odd_part = pair_view[..., 1]
    turned = jnp.stack([even_part * cos_tab - odd_part * sin_tab, even_part * sin_tab + odd_part * cos_tab], axis=-1)
    return turned.reshape(values.shape)


def reference(hidden, positions, doc_ids, norm_gain, w_query, w_key, w_value, w_out, grad_out):
    group_size = NUM_HEADS // NUM_KV_HEADS
    attn_scale = HEAD_DIM ** -0.5
    inv_freq = ROPE_BASE ** (-jnp.arange(0, HEAD_DIM, 2, dtype=jnp.float32) / HEAD_DIM)
    angles = positions.astype(jnp.float32)[:, :, None] * inv_freq
    cos_tab = jnp.cos(angles)[:, :, None, :]
    sin_tab = jnp.sin(angles)[:, :, None, :]
    token_idx = jnp.arange(SEQ_LEN, dtype=jnp.int32)
    allowed = (doc_ids[:, :, None] == doc_ids[:, None, :]) & (token_idx[None, :] <= token_idx[:, None])[None]

    def head_group(operands):
        query_grp, key_grp, value_grp = operands
        scores = jnp.einsum('bqgd,bkd->bgqk', query_grp, key_grp) * attn_scale
        scores = jnp.where(allowed[:, None], scores, -1e30)
        attn_probs = snap_bf16(jax.nn.softmax(scores, axis=-1))
        return snap_bf16(jnp.einsum('bgqk,bkd->bqgd', attn_probs, value_grp))

    def forward(hidden_f32, gain_f32, wq_f32, wk_f32, wv_f32, wo_f32):
        mean_sq = jnp.mean(hidden_f32 * hidden_f32, axis=-1, keepdims=True)
        normed = snap_bf16(hidden_f32 * lax.rsqrt(mean_sq + NORM_EPS) * gain_f32)
        query_raw = jnp.dot(normed, wq_f32).reshape(BATCH_ROWS, SEQ_LEN, NUM_HEADS, HEAD_DIM)
        key_raw = jnp.dot(normed, wk_f32).reshape(BATCH_ROWS, SEQ_LEN, NUM_KV_HEADS, HEAD_DIM)
        query_rot = snap_bf16(rotate_pairs(query_raw, cos_tab, sin_tab))
        key_rot = snap_bf16(rotate_pairs(key_raw, cos_tab, sin_tab))
        value_rows = snap_bf16(jnp.dot(normed, wv_f32)).reshape(BATCH_ROWS, SEQ_LEN, NUM_KV_HEADS, HEAD_DIM)
        query_groups = jnp.moveaxis(query_rot.reshape(BATCH_ROWS, SEQ_LEN, NUM_KV_HEADS, group_size, HEAD_DIM), 2, 0)
        heads_out = lax.map(jax.checkpoint(head_group), (query_groups, jnp.moveaxis(key_rot, 2, 0), jnp.moveaxis(value_rows, 2, 0)))
        heads_flat = jnp.moveaxis(heads_out, 0, 2).reshape(BATCH_ROWS, SEQ_LEN, NUM_HEADS * HEAD_DIM)
        attn_sum = snap_bf16(jnp.dot(heads_flat, wo_f32))
        return snap_bf16(hidden_f32 + attn_sum)

    attn_out, pullback = jax.vjp(forward, hidden.astype(jnp.float32), norm_gain.astype(jnp.float32), w_query.astype(jnp.float32), w_key.astype(jnp.float32), w_value.astype(jnp.float32), w_out.astype(jnp.float32))
    grad_list = pullback(grad_out.astype(jnp.float32))
    return (attn_out.astype(jnp.bfloat16), grad_list[0].astype(jnp.bfloat16), grad_list[1], grad_list[2], grad_list[3], grad_list[4], grad_list[5])
```

```python
import functools
import jax
import jax.numpy as jnp
from jax import lax
from jax.experimental import pallas as pl
from jax.experimental.pallas import tpu as pltpu
from jax.sharding import PartitionSpec as P

HEAD_DIM = 128
NORM_EPS = 1e-5
ROPE_BASE = 10000.0
F32 = jnp.float32
BF16 = jnp.bfloat16


def dot(a, b, ca, cb):
    return lax.dot_general(a, b, (((ca,), (cb,)), ((), ())), preferred_element_type=F32)


def after(value, gate):
    return lax.optimization_barrier((value, gate))[0]


def attention_kernel(n_q, half, ring, where_ref, qkv_ref, gh_ref, cos_ref, sin_ref, pos_ref, ho_ref, gqkv_ref, bias_ref):
    seq = qkv_ref.shape[0]
    D = HEAD_DIM
    scale = D ** -0.5
    chip, core = where_ref[0], where_ref[1]

    def token_index(idx):
        slot = idx // (2 * half)
        side = (idx // half) % 2
        return ((chip + slot) % ring) * (2 * half) + ((core + side) % 2) * half + idx % half

    @pl.when(pl.program_id(0) == 0)
    def _():
        tok_q = token_index(lax.broadcasted_iota(jnp.int32, (seq, 1), 0))
        tok_k = token_index(lax.broadcasted_iota(jnp.int32, (1, seq), 1))
        first = tok_q - pos_ref[...]
        allowed = (tok_k <= tok_q) & (tok_k >= first)
        bias_ref[...] = jnp.where(allowed, 0.0, -1e30)

    cos_tab, sin_tab = cos_ref[...], sin_ref[...]
    even = lax.broadcasted_iota(jnp.int32, (seq, D), 1) % 2 == 0

    def swap(v):
        return jnp.where(even, pltpu.roll(v, D - 1, 1), pltpu.roll(v, 1, 1))

    def rope(v):
        return v * cos_tab + swap(v) * sin_tab

    def unrope(v):
        return v * cos_tab - swap(v) * sin_tab

    key = rope(qkv_ref[:, n_q * D:(n_q + 1) * D]).astype(BF16)
    val = qkv_ref[:, (n_q + 1) * D:].astype(BF16)
    grad_k = jnp.zeros((seq, D), F32)
    grad_v = jnp.zeros((seq, D), F32)
    for h in range(n_q):
        cols = slice(h * D, (h + 1) * D)
        query = rope(qkv_ref[:, cols]).astype(BF16)
        grad_o = gh_ref[:, cols]
        scores = dot(query, key, 1, 1) * scale + bias_ref[...]
        e = jnp.exp(scores - jnp.max(scores, axis=1, keepdims=True))
        probs = e * (1.0 / jnp.sum(e, axis=1, keepdims=True))
        probs_low = probs.astype(BF16)
        ho_ref[:, cols] = dot(probs_low, val, 1, 0).astype(BF16)
        grad_p = dot(grad_o, val, 1, 1)
        grad_v += dot(probs_low, grad_o, 0, 0)
        row_dot = jnp.sum(probs * grad_p, axis=1, keepdims=True)
        grad_s = (probs * (grad_p - row_dot) * scale).astype(BF16)
        gqkv_ref[:, cols] = unrope(dot(grad_s, key, 1, 0)).astype(BF16)
        grad_k += dot(grad_s, query, 0, 0)
    gqkv_ref[:, n_q * D:(n_q + 1) * D] = unrope(grad_k).astype(BF16)
    gqkv_ref[:, (n_q + 1) * D:] = grad_v.astype(BF16)


def attention(where, qkv, grad_heads, cos_tab, sin_tab, pos, n_q, half, ring):
    seq = qkv.shape[0]
    D = HEAD_DIM
    width = (n_q + 2) * D
    groups = qkv.shape[1] // width
    fixed = lambda g, w: (0, 0)
    col = lambda g, w: (0, g)
    flops = groups * n_q * 6 * 2 * seq * seq * D * 2
    return pl.pallas_call(
        functools.partial(attention_kernel, n_q, half, ring),
        grid_spec=pltpu.PrefetchScalarGridSpec(
            num_scalar_prefetch=1,
            grid=(groups,),
            in_specs=[
                pl.BlockSpec((seq, width), col),
                pl.BlockSpec((seq, n_q * D), col),
                pl.BlockSpec((seq, D), fixed),
                pl.BlockSpec((seq, D), fixed),
                pl.BlockSpec((seq, 1), fixed),
            ],
            out_specs=[pl.BlockSpec((seq, n_q * D), col), pl.BlockSpec((seq, width), col)],
            scratch_shapes=[pltpu.VMEM((seq, seq), F32)],
        ),
        out_shape=[
            jax.ShapeDtypeStruct((seq, groups * n_q * D), BF16),
            jax.ShapeDtypeStruct((seq, groups * width), BF16),
        ],
        compiler_params=pltpu.CompilerParams(dimension_semantics=("arbitrary",), vmem_limit_bytes=40 * 2**20),
        cost_estimate=pl.CostEstimate(flops=flops, bytes_accessed=12 * 2**20, transcendentals=groups * n_q * seq * seq),
    )(where, qkv, grad_heads, cos_tab, sin_tab, pos)


def solution(mesh):
    tp = mesh.shape['tp']
    ring = tp // 2
    assert ring == 4
    to_partner = [(t, t ^ 1) for t in range(tp)]
    to_right = [(t, (t + 2) % tp) for t in range(tp)]
    to_left = [(t, (t - 2) % tp) for t in range(tp)]
    to_far = [(t, (t + 4) % tp) for t in range(tp)]

    def partner(v):
        return lax.ppermute(v, 'tp', to_partner)

    def right(v):
        return lax.ppermute(v, 'tp', to_right)

    def left(v):
        return lax.ppermute(v, 'tp', to_left)

    def device_step(hidden, positions, doc_ids, norm_gain, w_query, w_key, w_value, w_out, grad_out):
        me = lax.axis_index('tp')
        core, chip = me % 2, me // 2
        rows, half, width = hidden.shape
        mine = rows // 2
        n_q = w_query.shape[1] // w_key.shape[1]
        where = jnp.stack([chip, core]).astype(jnp.int32)

        hidden_f = hidden.astype(F32)
        inv_rms = lax.rsqrt(jnp.mean(hidden_f * hidden_f, axis=-1, keepdims=True) + NORM_EPS)
        gain_f = norm_gain.astype(F32)
        normed = (hidden_f * inv_rms * gain_f).astype(BF16)

        def split(v):
            own = lax.dynamic_slice_in_dim(v, core * mine, mine, 0)
            other = lax.dynamic_slice_in_dim(v, (1 - core) * mine, mine, 0)
            return [own[r] for r in range(mine)], [other[r] for r in range(mine)]

        n_own, n_other = split(normed)
        g_own, g_other = split(grad_out)

        def gather(own, other, gate):
            if gate is not None:
                own, other = after((own, other), gate)
            h0, h1 = own, partner(other)
            l0, r1 = right(h0), left(h1)
            l1, r0 = right(h1), left(h0)
            far0, far1 = right(l0), left(r1)
            return jnp.concatenate([h0, h1, r0, r1, far0, far1, l0, l1], axis=0), (l1, r0)

        n_full, g_full = [], []
        gate = None
        for r in range(mine):
            nf, _ = gather(n_own[r], n_other[r], gate)
            gf, gate_next = gather(g_own[r], g_other[r], gate)
            gate = gate_next
            n_full.append(nf)
            g_full.append(gf)

        w_mine = jnp.concatenate([w_query, w_key, w_value], axis=1)
        w_cat = jnp.concatenate([w_mine, partner(w_mine)], axis=1)
        wo_cat = jnp.concatenate([w_out, partner(w_out)], axis=0)

        pos_all = lax.all_gather(positions, 'tp', axis=0).reshape(ring, 2, rows, half)
        pos_all = jnp.concatenate([pos_all, pos_all], axis=0)
        pos_all = lax.dynamic_slice_in_dim(pos_all, chip, ring, 0)
        pos_all = jnp.concatenate([pos_all, pos_all], axis=1)
        pos_all = lax.dynamic_slice_in_dim(pos_all, core, 2, 1)
        pos_all = lax.dynamic_slice_in_dim(pos_all, core * mine, mine, 2)
        pos_rows = jnp.moveaxis(pos_all, 2, 0).reshape(mine, ring * 2 * half)
        lane = jnp.arange(HEAD_DIM)
        inv_freq = ROPE_BASE ** (-(2 * (lane // 2)).astype(F32) / HEAD_DIM)
        angles = pos_rows.astype(F32)[:, :, None] * inv_freq
        cos_tab = jnp.cos(angles)
        sin_tab = jnp.sin(angles) * jnp.where(lane % 2 == 0, -1.0, 1.0)

        def sum_scatter(lhs, rhs, cr):
            b = 2 * half
            p2 = dot(lhs[2 * b:3 * b], rhs, 1, cr).astype(BF16)
            from_left, from_right = right(p2[:half]), left(p2[half:])
            zero = jnp.zeros((half, width), BF16)
            p1 = (dot(lhs[b:2 * b], rhs, 1, cr) + jnp.concatenate([from_left, zero]).astype(F32)).astype(BF16)
            p3 = (dot(lhs[3 * b:], rhs, 1, cr) + jnp.concatenate([zero, from_right]).astype(F32)).astype(BF16)
            last_left, last_right = right(p1), left(p3)
            return (dot(lhs[:b], rhs, 1, cr) + last_left.astype(F32) + last_right.astype(F32)).astype(BF16)

        heads, grads, attn_rows, gn_rows = [], [], [], []
        for r in range(mine):
            qkv = dot(n_full[r], w_cat, 1, 0)
            grad_heads = dot(g_full[r], wo_cat, 1, 1).astype(BF16)
            ho, gqkv = attention(where, qkv, grad_heads, cos_tab[r], sin_tab[r], pos_rows[r][:, None], n_q, half, ring)
            heads.append(ho)
            grads.append(gqkv)
            attn_rows.append(sum_scatter(ho, wo_cat, 0))
            gn_rows.append(sum_scatter(gqkv, w_cat, 1))

        n_wide = w_mine.shape[1]
        o_wide = w_out.shape[0]

        def over_rows(lefts, rights):
            total = dot(lefts[0], rights[0], 0, 0)
            for a, b in zip(lefts[1:], rights[1:]):
                total = total + dot(a, b, 0, 0)
            return total

        gw_other = partner(over_rows(n_full, [g[:, n_wide:] for g in grads]).astype(BF16))
        gwo_other = partner(over_rows([h[:, o_wide:] for h in heads], g_full).astype(BF16))
        gw_mine = over_rows(n_full, [g[:, :n_wide] for g in grads]) + gw_other.astype(F32)
        q_wide, k_wide = w_query.shape[1], w_key.shape[1]
        grad_wq = gw_mine[:, :q_wide]
        grad_wk = gw_mine[:, q_wide:q_wide + k_wide]
        grad_wv = gw_mine[:, q_wide + k_wide:]
        grad_w_out = over_rows([h[:, :o_wide] for h in heads], g_full) + gwo_other.astype(F32)

        def to_tokens(parts):
            own = jnp.stack([p[:half] for p in parts])
            other = jnp.stack([partner(p[half:]) for p in parts])
            return lax.dynamic_slice_in_dim(jnp.concatenate([own, other, own], axis=0), core * mine, rows, 0)

        attn_out = hidden + to_tokens(attn_rows)
        grad_normed = to_tokens(gn_rows).astype(F32)
        gain_in = grad_normed * gain_f
        gain_part = jnp.sum(grad_normed * hidden_f * inv_rms, axis=(0, 1))
        mean_term = jnp.mean(gain_in * hidden_f, axis=-1, keepdims=True)
        grad_norm_in = inv_rms * gain_in - hidden_f * (inv_rms * inv_rms * inv_rms) * mean_term
        grad_hidden = (grad_out.astype(F32) + grad_norm_in).astype(BF16)
        pair = gain_part + partner(gain_part)
        far = lax.ppermute(pair, 'tp', to_far)
        grad_gain = (pair + far) + (right(pair) + left(pair))
        return (attn_out, grad_hidden, grad_gain, grad_wq, grad_wk, grad_wv, grad_w_out)

    row_spec = P('dp', 'tp', None)
    tok_spec = P('dp', 'tp')
    col_spec = P(None, 'tp')
    return jax.shard_map(
        device_step, mesh=mesh,
        in_specs=(row_spec, tok_spec, tok_spec, P(), col_spec, col_spec, col_spec, P('tp', None), row_spec),
        out_specs=(row_spec, row_spec, P('dp'), P('dp', 'tp'), P('dp', 'tp'), P('dp', 'tp'), P(('dp', 'tp'), None)),
        check_vma=False)
```
